128 devices in a mesh: branch: 2 (over y_lo), res: 64 (over y_hi, z, x, core).
Axes of the slice: x: 4, y: 4 (y_hi: 2, y_lo: 2; y = y_hi * 2 + y_lo), z: 4, core: 2. Of those that a mesh axis runs over, the one named last changes fastest.
Arguments:
- alignment_representation: float32 [128, 384, 256], P(None, 'res'), may hold values from -6 to 6
- pairwise_state: float32 [384, 384, 128], P('res'), may hold values from -6 to 6
- alignment_mask: int32 [128, 384], P(None, 'res'), may hold values from 0 to 1, as said below
- residue_present_mask: int32 [384], P('res'), may hold values from 0 to 1, as said below
- row_projection_weight: float32 [4, 256, 256], replicated
- lateral_result_coeffs: float32 [256, 256], replicated, may hold values from -1.5 to 1.5
- pair_bias_weight: float32 [128, 8], replicated, may hold values from -0.75 to 0.75
- first_operand_coeffs: float32 [256, 32], replicated, may hold values from -0.375 to 0.375
- other_operand_coeffs: float32 [256, 32], replicated, may hold values from -0.375 to 0.375
- outer_output_weight: float32 [1024, 128], replicated, may hold values from -2 to 2
- starting_projection_weight: float32 [4, 128, 128], replicated
- starting_bias_weight: float32 [128, 4], replicated, may hold values from -0.75 to 0.75
- starting_output_weight: float32 [128, 128], replicated, may hold values from -2 to 2
- ending_projection_weight: float32 [4, 128, 128], replicated
- ending_bias_weight: float32 [128, 4], replicated, may hold values from -0.75 to 0.75
- ending_output_weight: float32 [128, 128], replicated, may hold values from -2 to 2
Outputs:
- alignment_output: float32 [128, 384, 256], P('branch', 'res')
- pairwise_output: float32 [384, 384, 128], P('res', None, 'branch')
The draws below stay inside these ranges and needn't reach their ends.
Inputs may be any that keep to these rules, and one draw needn't show every extreme that they name: residue_present_mask is 1 on the first L residues and 0 on the rest, for a drawn L from 192 to 384. alignment_mask[s, r] is 1 exactly where s is below a drawn count from 32 to 128 and residue_present_mask[r] is 1.
All inputs are finite; a program needn't handle non-finite values.
Results may differ from the reference program's by a relative error of at most 0.0003.
Values sent between devices are 32-bit elements; how exact they have to be, the bound alone decides.
No kernel may reach another device: no remote copies, remote signals or barrier semaphores. Data moves between devices by JAX's collectives and lax.ppermute only.
A program may use at most 128 MiB of HBM per device.

```python
import math
import jax
import jax.numpy as jnp
from jax import lax

ALIGNED_FEATURES = 256
C_Z = 128
ATTEND_HEADS = 8
HEADS_Z = 4
PRODUCT_WIDTH = 32
ALIGNED_CHAINS = 128
CUT_AMINO_COUNT = 384


def mask_counts(key):
    starting_amount = jax.random.fold_in(key, 7)
    live_res = jax.random.randint(jax.random.fold_in(starting_amount, 1), (), CUT_AMINO_COUNT // 2, CUT_AMINO_COUNT + 1)
    valid_chain_indicator = jax.random.randint(jax.random.fold_in(starting_amount, 2), (), ALIGNED_CHAINS // 4, ALIGNED_CHAINS + 1)
    return (live_res, valid_chain_indicator)


def draw_residue_present_mask(key, part):
    live_res, valid_chain_indicator = mask_counts(key)
    return (jnp.arange(CUT_AMINO_COUNT) < live_res).astype(jnp.int32)


def draw_alignment_mask(key, part):
    live_res, valid_chain_indicator = mask_counts(key)
    chain_share_slice = jnp.arange(ALIGNED_CHAINS)[:, None] < valid_chain_indicator
    res_part = jnp.arange(CUT_AMINO_COUNT)[None, :] < live_res
    return (chain_share_slice & res_part).astype(jnp.int32)


def rescaled_mapping(key, salt, channels):
    own_key = jax.random.fold_in(key, salt)
    starting_amount = jax.random.normal(jax.random.fold_in(own_key, 1), (4, channels, channels), jnp.float32) / math.sqrt(channels)
    return starting_amount


def draw_row_projection_weight(key, part):
    return rescaled_mapping(key, 101, ALIGNED_FEATURES)


def draw_starting_projection_weight(key, part):
    return rescaled_mapping(key, 202, C_Z)


def draw_ending_projection_weight(key, part):
    return rescaled_mapping(key, 303, C_Z)


def block_levels(rng, shape, shards, low, top_value):
    def one(axis_at, shards_of):
        draws = jax.random.uniform(jax.random.fold_in(jax.random.fold_in(rng, 6), axis_at), (shards_of,), jnp.float32, low / len(shards), top_value / len(shards))
        return jnp.repeat(jnp.exp(draws), shape[axis_at] // shards_of).reshape((-1,) + (1,) * (len(shape) - axis_at - 1))

    level = one(*shards[0])
    for cut in shards[1:]:
        level = level * one(*cut)
    return level


def normal_values(key, shape, width, limit, split=(), kind=jnp.bfloat16):
    level = block_levels(key, shape, split, -0.22, 0.18) if split else 1.0
    result = jax.random.normal(key, shape, jnp.float32) * width * level
    return jnp.minimum(jnp.maximum(result, -limit), limit).astype(kind)


def setup_inputs(seed: int = 0) -> dict:
    key_of = jax.random.split(jax.random.key(seed), 17)
    alignment_representation = normal_values(key_of[0], (ALIGNED_CHAINS, CUT_AMINO_COUNT, ALIGNED_FEATURES), 1.0, 6.0, ((1, 64),), jnp.float32)
    pairwise_state = normal_values(key_of[1], (CUT_AMINO_COUNT, CUT_AMINO_COUNT, C_Z), 1.0, 6.0, ((0, 64),), jnp.float32)
    alignment_mask = draw_alignment_mask(jax.random.fold_in(key_of[16], 71), 0)
    residue_present_mask = draw_residue_present_mask(jax.random.fold_in(key_of[16], 71), 0)
    row_projection_weight = draw_row_projection_weight(jax.random.fold_in(key_of[16], 71), 0)
    lateral_result_coeffs = normal_values(key_of[5], (ALIGNED_FEATURES, ALIGNED_FEATURES), (ALIGNED_FEATURES // 16) ** -0.5, 1.5, (), jnp.float32)
    pair_bias_weight = normal_values(key_of[6], (C_Z, ATTEND_HEADS), (C_Z // 2) ** -0.5, 0.75, (), jnp.float32)
    first_operand_coeffs = normal_values(key_of[7], (ALIGNED_FEATURES, PRODUCT_WIDTH), ALIGNED_FEATURES ** -0.5, 0.375, (), jnp.float32)
    other_operand_coeffs = normal_values(key_of[8], (ALIGNED_FEATURES, PRODUCT_WIDTH), ALIGNED_FEATURES ** -0.5, 0.375, (), jnp.float32)
    outer_output_weight = normal_values(key_of[9], (PRODUCT_WIDTH * PRODUCT_WIDTH, C_Z), (PRODUCT_WIDTH // 4) ** -0.5, 2.0, (), jnp.float32)
    starting_projection_weight = draw_starting_projection_weight(jax.random.fold_in(key_of[16], 71), 0)
    starting_bias_weight = normal_values(key_of[11], (C_Z, HEADS_Z), (C_Z // 2) ** -0.5, 0.75, (), jnp.float32)
    starting_output_weight = normal_values(key_of[12], (C_Z, C_Z), (C_Z // 16) ** -0.5, 2.0, (), jnp.float32)
    ending_projection_weight = draw_ending_projection_weight(jax.random.fold_in(key_of[16], 71), 0)
    ending_bias_weight = normal_values(key_of[14], (C_Z, HEADS_Z), (C_Z // 2) ** -0.5, 0.75, (), jnp.float32)
    ending_output_weight = normal_values(key_of[15], (C_Z, C_Z), (C_Z // 16) ** -0.5, 2.0, (), jnp.float32)
    return {"alignment_representation": alignment_representation, "pairwise_state": pairwise_state, "alignment_mask": alignment_mask, "residue_present_mask": residue_present_mask, "row_projection_weight": row_projection_weight, "lateral_result_coeffs": lateral_result_coeffs, "pair_bias_weight": pair_bias_weight, "first_operand_coeffs": first_operand_coeffs, "other_operand_coeffs": other_operand_coeffs, "outer_output_weight": outer_output_weight, "starting_projection_weight": starting_projection_weight, "starting_bias_weight": starting_bias_weight, "starting_output_weight": starting_output_weight, "ending_projection_weight": ending_projection_weight, "ending_bias_weight": ending_bias_weight, "ending_output_weight": ending_output_weight}


highest = lax.Precision.HIGHEST
epsilon = 1e-05
masked_score = -1000000000.0

def layer_normalize(values):
    centred = values - lax.optimization_barrier(jnp.mean(values, axis=-1, keepdims=True))
    variance = lax.optimization_barrier(jnp.mean(centred * centred, axis=-1, keepdims=True))
    return centred * lax.rsqrt(variance + epsilon)

def linear_project(values, weight):
    return jnp.dot(values, weight, precision=highest, preferred_element_type=jnp.float32)

def attend(query_matrix, key_matrix, value_matrix, gate_matrix, score_bias, live_keys, head_count):
    head_width = query_matrix.shape[-1] // head_count
    shaped_q = query_matrix.reshape(query_matrix.shape[0], head_count, head_width)
    shaped_k = key_matrix.reshape(key_matrix.shape[0], head_count, head_width)
    shaped_v = value_matrix.reshape(value_matrix.shape[0], head_count, head_width)
    scores = jnp.einsum('qhd,khd->hqk', shaped_q, shaped_k, precision=highest) / math.sqrt(head_width) + score_bias
    scores = jnp.where(live_keys[None, None, :], scores, masked_score)
    scores = scores - lax.optimization_barrier(jnp.max(scores, axis=-1, keepdims=True))
    weights = jnp.exp(scores)
    weights = weights / lax.optimization_barrier(jnp.sum(weights, axis=-1, keepdims=True))
    mixture = jnp.einsum('hqk,khd->qhd', weights, shaped_v, precision=highest)
    return jax.nn.sigmoid(gate_matrix) * mixture.reshape(query_matrix.shape[0], head_count * head_width)

def factor_matrix(normed, float_mask, weight):
    return jnp.transpose(linear_project(normed, weight) * float_mask[:, :, None], (1, 2, 0))

def outer_block(left_matrix, mask_rows, right_all, mask_all, out_weight):
    residues, factor_width, sequences = right_all.shape

    def one_row(operands):
        row_left, row_mask = operands
        outer_sum = jnp.einsum('cs,jes->jce', row_left, right_all, precision=highest)
        outer_sum = outer_sum.reshape(residues, factor_width * factor_width)
        intersection = jnp.einsum('ns,s->n', mask_all, row_mask, precision=highest)
        return linear_project(outer_sum, out_weight) / jnp.maximum(intersection, 1.0)[:, None]
    return lax.map(one_row, (left_matrix, mask_rows))

def starting_change(field, proj, bias_weight, out_weight, live_keys):
    normed = layer_normalize(field)
    score_bias = jnp.einsum('ijc,ch->hij', normed, bias_weight, precision=highest)
    query_matrix = linear_project(normed, proj[0])
    key_matrix = linear_project(normed, proj[1])
    value_matrix = linear_project(normed, proj[2])
    gate_matrix = linear_project(normed, proj[3])

    def one_row(operands):
        return attend(operands[0], operands[1], operands[2], operands[3], score_bias, live_keys, HEADS_Z)
    gated_output = lax.map(one_row, (query_matrix, key_matrix, value_matrix, gate_matrix))
    return linear_project(gated_output, out_weight)

def reference(alignment_representation, pairwise_state, alignment_mask, residue_present_mask, row_projection_weight, lateral_result_coeffs, pair_bias_weight, first_operand_coeffs, other_operand_coeffs, outer_output_weight, starting_projection_weight, starting_bias_weight, starting_output_weight, ending_projection_weight, ending_bias_weight, ending_output_weight):
    normed_alignment = layer_normalize(alignment_representation)
    row_bias = jnp.einsum('ijc,ch->hij', layer_normalize(pairwise_state), pair_bias_weight, precision=highest)
    query_matrix = linear_project(normed_alignment, row_projection_weight[0])
    key_matrix = linear_project(normed_alignment, row_projection_weight[1])
    value_matrix = linear_project(normed_alignment, row_projection_weight[2])
    gate_matrix = linear_project(normed_alignment, row_projection_weight[3])
    sequence_present = alignment_mask > 0

    def one_sequence(operands):
        return attend(operands[0], operands[1], operands[2], operands[3], row_bias, operands[4], ATTEND_HEADS)
    gated_output = lax.map(one_sequence, (query_matrix, key_matrix, value_matrix, gate_matrix, sequence_present))
    alignment_output = alignment_representation + linear_project(gated_output, lateral_result_coeffs)
    float_mask = alignment_mask.astype(jnp.float32)
    left_matrix = factor_matrix(normed_alignment, float_mask, first_operand_coeffs)
    right_matrix = factor_matrix(normed_alignment, float_mask, other_operand_coeffs)
    mask_rows = jnp.transpose(float_mask)
    update = outer_block(left_matrix, mask_rows, right_matrix, mask_rows, outer_output_weight)
    pair_one = pairwise_state + update
    live_keys = residue_present_mask > 0
    pairwise_second = pair_one + starting_change(pair_one, starting_projection_weight, starting_bias_weight, starting_output_weight, live_keys)
    flipped = jnp.transpose(pairwise_second, (1, 0, 2))
    ending = starting_change(flipped, ending_projection_weight, ending_bias_weight, ending_output_weight, live_keys)
    pairwise_output = pairwise_second + jnp.transpose(ending, (1, 0, 2))
    return (alignment_output, pairwise_output)
```

```python
import math

import jax
import jax.numpy as jnp
from jax import lax
from jax.experimental import pallas as pl
from jax.experimental.pallas import tpu as pltpu
from jax.sharding import Mesh
from jax.sharding import PartitionSpec as P

RES = ("y", "z", "x", "c")
CHIPS = ("y", "z", "x")
EPS = 1e-05
MASKED = -1000000000.0
N = 384
F32 = jnp.float32
BF16 = jnp.bfloat16
VMEM = pl.BlockSpec(memory_space=pltpu.VMEM)
SMEM = pl.BlockSpec(memory_space=pltpu.SMEM)


def halves(x):
    hi = x.astype(BF16)
    return hi, (x - hi.astype(F32)).astype(BF16)


def dg(a, b, ca, cb):
    return lax.dot_general(a, b, (((ca,), (cb,)), ((), ())), preferred_element_type=F32)


def dot3(a, b, ca=1, cb=0):
    return dg(a[0], b[0], ca, cb) + (dg(a[0], b[1], ca, cb) + dg(a[1], b[0], ca, cb))


def normalize(x):
    centred = x - jnp.mean(x, axis=-1, keepdims=True)
    variance = jnp.mean(centred * centred, axis=-1, keepdims=True)
    return centred * lax.rsqrt(variance + EPS)


def call(body, out_shape, args, smem=0, scratch=(), flops=10**9, name=None):
    specs = [SMEM] * smem + [VMEM] * (len(args) - smem)
    single = not isinstance(out_shape, (list, tuple))
    return pl.pallas_call(
        body,
        out_shape=out_shape,
        in_specs=specs,
        out_specs=VMEM if single else [VMEM] * len(out_shape),
        scratch_shapes=list(scratch),
        compiler_params=pltpu.CompilerParams(vmem_limit_bytes=60000 * 1024),
        cost_estimate=pl.CostEstimate(flops=flops, bytes_accessed=4 * 10**6, transcendentals=0),
        name=name,
    )(*args)


def shaped(*dims):
    return jax.ShapeDtypeStruct(dims, F32)


def shift(value, axis, by):
    count = lax.axis_size(axis)
    return lax.ppermute(value, axis, [(i, (i + by) % count) for i in range(count)])


def factor_body(branch_ref, msa_ref, mask_ref, live_ref, whi_ref, wlo_ref, left_ref, right_ref, seq_ref):
    weights = (whi_ref[...], wlo_ref[...])
    first = pl.multiple_of(branch_ref[0] * 64, 64)
    left_ref[192:200, :] = jnp.zeros((8, 128), F32)
    right_ref[192:200, :] = jnp.zeros((8, 128), F32)
    for i in range(6):
        seq_ref[:, i, :] = normalize(msa_ref[pl.ds(first, 64), i, :])
        normed = normalize(msa_ref[:, i, :])
        row = mask_ref[i : i + 1, :]
        both = dot3(weights, halves(normed), 0, 1) * row
        left_ref[32 * i : 32 * i + 32, :] = both[:32]
        right_ref[32 * i : 32 * i + 32, :] = both[32:]
        left_ref[192 + i : 193 + i, :] = row
        right_ref[192 + i : 193 + i, :] = row
    seq_ref[:, 6:8, :] = live_ref[...]


def rowbias_body(pair_ref, whi_ref, wlo_ref, out_ref):
    weights = (whi_ref[...], wlo_ref[...])
    for i in range(6):
        rows = dot3(weights, halves(normalize(pair_ref[i])), 1, 1)
        for h in range(8):
            out_ref[h, i : i + 1, :] = rows[h : h + 1]
    out_ref[:, 6:8, :] = jnp.zeros((8, 2, N), F32)


def outer_body(
    at_ref, lown_ref, lpar_ref, r_ref, whi_ref, wlo_ref,
    o0_ref, o1_ref, o2_ref, o3_ref, par_ref,
    rhi_ref, rlo_ref, lhi_ref, llo_ref, q_ref, acc_ref, mj_ref, mi_ref,
):
    y, z = at_ref[0], at_ref[1]
    for a in range(8):
        dy = lax.rem(y - a // 4 + 2, 2)
        dz = lax.rem(z - a % 4 + 4, 4)
        block = r_ref[dz, dy]
        hi, lo = halves(block[:192])
        rhi_ref[192 * a : 192 * a + 192, :] = hi
        rlo_ref[192 * a : 192 * a + 192, :] = lo
        mj_ref[6 * a : 6 * a + 6, :] = block[192:198]
    for d in range(8):
        block = (lown_ref if d < 4 else lpar_ref)[d % 4]
        hi, lo = halves(block[:192])
        lhi_ref[192 * d : 192 * d + 192, :] = hi
        llo_ref[192 * d : 192 * d + 192, :] = lo
        mi_ref[6 * d : 6 * d + 6, :] = block[192:198]

    @pl.loop(0, 12)
    def _(g):
        at = pl.ds(pl.multiple_of(g * 128, 128), 128)
        lg = (lhi_ref[at, :], llo_ref[at, :])
        q_ref[g] = dot3((rhi_ref[...], rlo_ref[...]), lg, 1, 1)

    acc_ref[...] = jnp.zeros_like(acc_ref)

    @pl.loop(0, 16)
    def _(e):
        rows = []
        for g in range(12):
            rows.append(
                jnp.concatenate(
                    [q_ref[g, pl.ds(2 * e, 48, stride=32), :], q_ref[g, pl.ds(2 * e + 1, 48, stride=32), :]],
                    axis=1,
                )
            )
        both = halves(jnp.concatenate(rows, axis=0))
        acc_ref[...] += dot3(both, (whi_ref[e], wlo_ref[e]))

    shared = dg(mj_ref[...].astype(BF16), mi_ref[...].astype(BF16), 1, 1)
    inverse = 1.0 / jnp.maximum(shared, 1.0)
    outs = (o0_ref, o1_ref, o2_ref, o3_ref)
    for n in range(48):
        g, q = n // 4, n % 4
        tile = acc_ref[48 * g : 48 * g + 48, 128 * q : 128 * q + 128] * inverse[:, n : n + 1]
        if n < 24:
            outs[n // 6][n % 6] = tile
        else:
            par_ref[(n - 24) // 6, n % 6] = tile


def join_body(at_ref, pieces_ref, pair_ref, whi_ref, wlo_ref, one_ref, bias_ref):
    x, c = at_ref[2], at_ref[3]
    weights = (whi_ref[...], wlo_ref[...])
    for i in range(6):
        for k in range(8):
            dx = lax.rem(k // 2 - x + 4, 4)
            dc = lax.rem(k % 2 - c + 2, 2)
            piece = pieces_ref[dc * 4 + dx, i]
            for a in range(8):
                to = 48 * a + 6 * k
                one_ref[i, to : to + 6, :] = pair_ref[i, to : to + 6, :] + piece[6 * a : 6 * a + 6]
        rows = dot3(weights, halves(normalize(one_ref[i])), 1, 1)
        for h in range(4):
            bias_ref[6 * h + i : 6 * h + i + 1, :] = rows[h : h + 1]


def gather_bias(c, own_ref, par_ref, bias_ref, turned):
    for h in range(4):
        for a in range(32):
            own = own_ref[a, 6 * h : 6 * h + 6, :]
            par = par_ref[a, 6 * h : 6 * h + 6, :]
            bias_ref[h, 12 * a : 12 * a + 6, :] = jnp.where(c == 0, own, par)
            bias_ref[h, 12 * a + 6 : 12 * a + 12, :] = jnp.where(c == 0, par, own)
        if turned:
            bias_ref[h] = bias_ref[h].T


def mix_heads(q, k, v, bias_of, live):
    lane = lax.broadcasted_iota(jnp.int32, (N, 128), 1)
    khi, klo = halves(k)
    vhi, vlo = halves(v)
    keys = jnp.concatenate([khi, khi], axis=1)
    values = jnp.concatenate([vhi, vlo], axis=1)
    out = jnp.zeros((N, 128), F32)
    for h in range(4):
        here = lane // 32 == h
        qhi, qlo = halves(jnp.where(here, q, 0.0))
        scores = dg(jnp.concatenate([qhi, qlo], axis=1), keys, 1, 1) + dg(qhi, klo, 1, 1)
        scores = jnp.where(live, scores + bias_of(h), MASKED)
        weights = jnp.exp(scores - jnp.max(scores, axis=-1, keepdims=True))
        total = jnp.sum(weights, axis=-1, keepdims=True)
        whi, wlo = halves(weights)
        mixed = dg(whi, values, 1, 0)
        mixed = mixed[:, :128] + mixed[:, 128:] + dg(wlo, vhi, 1, 0)
        out = jnp.where(here, mixed / total, out)
    return out


def triangle(normed, weights, bias_ref, live):
    qkvg = dot3(halves(normed), weights)
    mixed = mix_heads(
        qkvg[:, :128] * (1.0 / math.sqrt(32.0)),
        qkvg[:, 128:256],
        qkvg[:, 256:384],
        lambda h: bias_ref[h],
        live,
    )
    return halves(jax.nn.sigmoid(qkvg[:, 384:]) * mixed)


def start_body(
    at_ref, one_ref, own_ref, par_ref, live_ref, phi_ref, plo_ref, ohi_ref, olo_ref, bhi_ref, blo_ref,
    two_ref, normed_ref, out_ref, bias_ref,
):
    gather_bias(at_ref[3], own_ref, par_ref, bias_ref, False)
    live = live_ref[...] > 0.5
    weights = (phi_ref[...], plo_ref[...])
    out_weights = (ohi_ref[...], olo_ref[...])
    bias_weights = (bhi_ref[...], blo_ref[...])

    @pl.loop(0, 6)
    def _(i):
        one = one_ref[i]
        gated = triangle(normalize(one), weights, bias_ref, live)
        two = one + dot3(gated, out_weights)
        two_ref[i] = two
        normed = normalize(two)
        normed_ref[i] = normed
        out_ref[i] = dot3(bias_weights, halves(normed), 1, 1)


def end_body(
    at_ref, cols_ref, own_ref, par_ref, live_ref, phi_ref, plo_ref, ohi_ref, olo_ref, out_ref, bias_ref
):
    gather_bias(at_ref[3], own_ref, par_ref, bias_ref, True)
    live = live_ref[...] > 0.5
    weights = (phi_ref[...], plo_ref[...])

    @pl.loop(0, 3)
    def _(p):
        total = jnp.zeros((N, 128), F32)
        for half in range(2):
            normed = cols_ref[pl.ds(2 * p + half, N, stride=6), :]
            gated = triangle(normed, weights, bias_ref, live)
            total = total + dot3(gated, (ohi_ref[half], olo_ref[half]))
        out_ref[p] = total


def row_body(seq_ref, bias_in, live_ref, phi_ref, plo_ref, ohi_ref, olo_ref, out_ref, bias_ref, y_ref):
    live = live_ref[...] > 0.5
    seq = halves(seq_ref[...])
    for part in range(4):
        y_ref[part] = dot3(seq, (phi_ref[part], plo_ref[part]))
    total = jnp.zeros((N, 256), F32)
    for group in range(2):
        at = slice(128 * group, 128 * group + 128)
        for h in range(4):
            for r in range(64):
                bias_ref[h, 6 * r : 6 * r + 6, :] = bias_in[r, 4 * group + h, 0:6, :]
        mixed = mix_heads(
            y_ref[0, :, at] * (1.0 / math.sqrt(32.0)), y_ref[1, :, at], y_ref[2, :, at], lambda h: bias_ref[h], live
        )
        gated = halves(jax.nn.sigmoid(y_ref[3, :, at]) * mixed)
        total = total + dot3(gated, (ohi_ref[at, :], olo_ref[at, :]))
    out_ref[...] = total


def block_diagonal(out_weight):
    by_e = out_weight.reshape(32, 32, 128).transpose(1, 0, 2)
    eye = jnp.eye(4, dtype=F32)
    spread = eye[None, :, None, :, None] * by_e[:, None, :, None, :]
    return spread.reshape(16, 256, 512)


def split_weights(w):
    hi = lax.reduce_precision(w, 8, 7)
    return hi.astype(BF16), (w - hi).astype(BF16)


def joined(projection):
    return jnp.concatenate([projection[k] for k in range(4)], axis=1)


def bias_rows(weight):
    return jnp.concatenate([weight.T, jnp.zeros((8 - weight.shape[1], weight.shape[0]), F32)], axis=0)


def per_device(
    msa, pair, msa_mask, residue_mask, row_proj, row_out, row_bias_w, first_w, other_w, outer_w,
    start_proj, start_bias_w, start_out, end_proj, end_bias_w, end_out,
):
    branch = lax.axis_index("b")
    at = jnp.stack([lax.axis_index(a) for a in RES]).astype(jnp.int32)
    mask = msa_mask.astype(F32)
    live6 = residue_mask.astype(F32)

    first = branch * 64
    own_mask = lax.dynamic_slice_in_dim(mask, first, 64, 0)
    flags = jnp.stack([own_mask, jnp.broadcast_to(live6, (64, 6))], axis=1)
    flags = jnp.pad(flags, ((0, 0), (0, 0), (0, 250)))
    lr = split_weights(jnp.concatenate([first_w, other_w], axis=1))
    left, right, seq_msg = call(
        factor_body,
        [shaped(200, 128), shaped(200, 128), shaped(64, 8, 256)],
        (branch.reshape(1).astype(jnp.int32), msa, mask.T, flags, *lr),
        smem=1, name="factors",
    )
    rows8 = call(rowbias_body, shaped(8, 8, N), (pair, *split_weights(row_bias_w.T)), name="rowbias")
    row_bias = lax.all_gather(rows8, RES, axis=0)

    lown = jnp.stack([left] + [shift(left, "x", k) for k in (1, 2, 3)])
    lpar = shift(lown, "c", 1)
    ry = jnp.stack([right, shift(right, "y", 1)])
    rz = jnp.stack([ry] + [shift(ry, "z", k) for k in (1, 2, 3)])

    tile = shaped(6, 48, 128)
    o0, o1, o2, o3, par = call(
        outer_body,
        [tile, tile, tile, tile, shaped(4, 6, 48, 128)],
        (at, lown, lpar, rz, *split_weights(block_diagonal(outer_w))),
        smem=1,
        scratch=[
            pltpu.VMEM((1536, 128), BF16),
            pltpu.VMEM((1536, 128), BF16),
            pltpu.VMEM((1536, 128), BF16),
            pltpu.VMEM((1536, 128), BF16),
            pltpu.VMEM((12, 1536, 128), F32),
            pltpu.VMEM((576, 512), F32),
            pltpu.VMEM((48, 128), F32),
            pltpu.VMEM((48, 128), F32),
        ],
        flops=4 * 10**9, name="outer",
    )
    got = shift(par, "c", 1)
    pieces = [o0] + [shift(o, "x", -k) for k, o in ((1, o1), (2, o2), (3, o3))]
    pieces += [got[0]] + [shift(got[k], "x", -k) for k in (1, 2, 3)]
    one, bias1 = call(
        join_body,
        [shaped(6, N, 128), shaped(24, N)],
        (at, jnp.stack(pieces), pair, *split_weights(bias_rows(start_bias_w))),
        smem=1, name="join",
    )

    def everywhere(rows):
        own = lax.all_to_all(jnp.broadcast_to(rows, (32, 24, N)), CHIPS, split_axis=0, concat_axis=0, tiled=True)
        return own, shift(own, "c", 1)

    seq_got = lax.all_to_all(seq_msg, RES, split_axis=0, concat_axis=0, tiled=True)
    seq = seq_got[:, :6].reshape(N, 256)
    seq_live = seq_got[:, 6, :6].reshape(1, N)
    live = seq_got[:, 7, :6].reshape(1, N)

    own1, par1 = everywhere(bias1)
    two, normed, rows2 = call(
        start_body,
        [shaped(6, N, 128), shaped(6, N, 128), shaped(6, 8, N)],
        (
            at, one, own1, par1, live, *split_weights(joined(start_proj)), *split_weights(start_out),
            *split_weights(bias_rows(end_bias_w)),
        ),
        smem=1, scratch=[pltpu.VMEM((4, N, N), F32)], flops=8 * 10**9, name="start",
    )
    bias2 = rows2[:, :4].transpose(1, 0, 2).reshape(24, N)
    own2, par2 = everywhere(bias2)
    msg = normed.reshape(6, 64, 6, 128).transpose(1, 0, 2, 3).reshape(64, 36, 128)
    cols = lax.all_to_all(msg, RES, split_axis=0, concat_axis=0, tiled=True).reshape(2304, 128)

    mixed = call(
        row_body,
        shaped(N, 256),
        (seq, row_bias, seq_live, *split_weights(row_proj), *split_weights(row_out)),
        scratch=[pltpu.VMEM((4, N, N), F32), pltpu.VMEM((4, N, 256), F32)],
        flops=4 * 10**9, name="rows",
    )
    msa_got = lax.all_to_all(mixed.reshape(64, 6, 256), RES, split_axis=0, concat_axis=0, tiled=True)
    msa_out = lax.dynamic_slice_in_dim(msa, first, 64, 0) + msa_got

    half = lax.dynamic_slice_in_dim(end_out, first, 64, 1)
    zero = jnp.zeros_like(half)
    halved = jnp.stack([jnp.concatenate([half, zero], axis=1), jnp.concatenate([zero, half], axis=1)])
    ended = call(
        end_body,
        shaped(3, N, 128),
        (at, cols, own2, par2, live, *split_weights(joined(end_proj)), *split_weights(halved)),
        smem=1, scratch=[pltpu.VMEM((4, N, N), F32)], flops=8 * 10**9, name="end",
    )
    back = ended.reshape(3, 64, 6, 128).transpose(1, 0, 2, 3).reshape(64, 18, 128)
    back = lax.all_to_all(back, RES, split_axis=0, concat_axis=0, tiled=True)
    back = back.reshape(64, 3, 6, 2, 64).transpose(2, 0, 1, 3, 4).reshape(6, N, 64)
    pair_out = lax.dynamic_slice_in_dim(two, first, 64, 2) + back
    return msa_out, pair_out


def solution(mesh):
    split = Mesh(mesh.devices.reshape(mesh.shape["branch"], 2, 4, 4, 2), ("b",) + RES)
    placed = (P(None, RES, None), P(RES, None, None), P(None, RES), P(RES)) + (P(),) * 12
    return jax.shard_map(
        per_device,
        mesh=split,
        in_specs=placed,
        out_specs=(P("b", RES, None), P(RES, None, "b")),
        check_vma=False,
    )
```
